32 devices in a mesh: row: 8 (over z, y), ta: 4 (over x, core).
Axes of the slice: x: 2, y: 2, z: 4, core: 2. Of those that a mesh axis runs over, the one named last changes fastest.
Arguments:
- rotation: float32 [16384, 16384], P(('row', 'ta')), may hold values from -0.046875 to 0.046875
- query_weight: bfloat16 [16384, 1536], P(('row', 'ta')), may hold values from -6 to 6
- key_weight: bfloat16 [16384, 512], P(('row', 'ta')), may hold values from -6 to 6
- value_weight: bfloat16 [16384, 512], P(('row', 'ta')), may hold values from -6 to 6
- head_rotation: float32 [4, 128, 128], P('ta'), may hold values from -0.5 to 0.5
Outputs:
- query_rotated: bfloat16 [16384, 1536], P('row', 'ta')
- key_rotated: bfloat16 [16384, 512], P('row', 'ta')
- value_rotated: bfloat16 [16384, 512], P('row', 'ta')
The draws below stay inside these ranges and needn't reach their ends.
All inputs are finite; a program needn't handle non-finite values.
Results may differ from the reference program's by a relative error of at most 0.0015.
Values may be sent and summed in bfloat16 or wider, within the bound.
A program may use at most 192 MiB of HBM per device.

```python
import jax
import jax.numpy as jnp
from jax import lax

D = 16384
HEAD = 128
KV_WIN = 4
QCOLS = 1536
KVCOLS = 512


def block_scale(key, extent, split, least, high):
    def one(dim, shards_of):
        steps = jax.random.uniform(jax.random.fold_in(jax.random.fold_in(key, 6), dim), (shards_of,), jnp.float32, least / len(split), high / len(split))
        return jnp.repeat(jnp.exp(steps), extent[dim] // shards_of).reshape((-1,) + (1,) * (len(extent) - dim - 1))

    loudness = one(*split[0])
    for cut in split[1:]:
        loudness = loudness * one(*cut)
    return loudness


def noise(rng, shape, width, bound, pieces=(), held_as=jnp.bfloat16):
    result = width * jax.random.normal(rng, shape, jnp.float32)
    if pieces:
        result = result * block_scale(rng, shape, pieces, -0.22, 0.18)
    return jnp.clip(result, -bound, bound).astype(held_as)


def setup_inputs(seed: int = 0) -> dict:
    seeds = jax.random.split(jax.random.key(seed), 6)
    rotation = noise(seeds[0], (D, D), D ** -0.5, 0.046875, ((0, 32),), jnp.float32)
    query_weight = noise(seeds[1], (D, QCOLS), 1.0, 6.0, ((0, 32),))
    key_weight = noise(seeds[2], (D, KVCOLS), 1.0, 6.0, ((0, 32),))
    value_weight = noise(seeds[3], (D, KVCOLS), 1.0, 6.0, ((0, 32),))
    head_rotation = noise(seeds[4], (KV_WIN, HEAD, HEAD), HEAD ** -0.5, 0.5, ((0, 4),), jnp.float32)
    return dict(rotation=rotation, query_weight=query_weight, key_weight=key_weight, value_weight=value_weight, head_rotation=head_rotation)


def rotate_weight(rotation, weight):
    return lax.dot_general(rotation, weight.astype(jnp.float32), (((0,), (0,)), ((), ())), precision=lax.Precision.HIGHEST, preferred_element_type=jnp.float32)


def reference(rotation, query_weight, key_weight, value_weight, head_rotation):
    query_rotated = rotate_weight(rotation, query_weight).astype(jnp.bfloat16)
    key_rotated = rotate_weight(rotation, key_weight).astype(jnp.bfloat16)
    value_mixed = rotate_weight(rotation, value_weight)
    per_head = value_mixed.reshape(D, KV_WIN, HEAD)
    turned = jnp.einsum("jhd,hde->jhe", per_head, head_rotation, precision=lax.Precision.HIGHEST)
    value_rotated = turned.reshape(D, KV_WIN * HEAD).astype(jnp.bfloat16)
    return query_rotated, key_rotated, value_rotated
```

```python
import functools

import jax
import jax.numpy as jnp
from jax import lax
from jax.experimental import pallas as pl
from jax.experimental.pallas import tpu as pltpu
from jax.sharding import PartitionSpec as P

CHUNKS = 8
LANES = 128
OFFSETS = ((0, 0), (0, 1), (1, 0), (1, 1))


def split_kernel(place, *refs):
    count = len(refs) // 2
    for source, out in zip(refs[:count], refs[count:]):
        block = source[...].T
        depth = block.shape[1]
        high = block.astype(jnp.bfloat16)
        out[:, :depth] = high
        out[:, depth:] = (block - high.astype(jnp.float32)).astype(jnp.bfloat16)


def split_chunk(rotation, place, layers, width, chunk, chunks):
    depth = rotation.shape[0]

    def incoming(dy, dx):
        def index(layer, place):
            y = (place[0] + dy) % 2
            x = (place[1] + dx) % 2
            return 0, ((layer * 2 + y) * 2 + x) * chunks + chunk

        return pl.BlockSpec((depth, width), index)

    return pl.pallas_call(
        split_kernel,
        out_shape=[jax.ShapeDtypeStruct((layers * width, 2 * depth), jnp.bfloat16)] * len(OFFSETS),
        grid_spec=pltpu.PrefetchScalarGridSpec(
            num_scalar_prefetch=1,
            grid=(layers,),
            in_specs=[incoming(*offset) for offset in OFFSETS],
            out_specs=[pl.BlockSpec((width, 2 * depth), lambda layer, place: (layer, 0))] * len(OFFSETS),
        ),
        cost_estimate=pl.CostEstimate(
            flops=0, bytes_accessed=8 * len(OFFSETS) * layers * width * depth, transcendentals=0
        ),
    )(place, *([rotation] * len(OFFSETS)))


def fold_kernel(*refs):
    count = len(OFFSETS)
    pieces, weight, out, high, low = refs[:count], refs[count], refs[count + 1], refs[count + 2], refs[count + 3]
    depth = weight.shape[0] // count
    for n, piece in enumerate(pieces):
        high[:, n * depth : (n + 1) * depth] = piece[:, :depth]
        low[:, n * depth : (n + 1) * depth] = piece[:, depth:]
    sides, layers, width, columns = out.shape
    tile = 2 * LANES if columns % (2 * LANES) == 0 else LANES
    for side in range(sides):

        @pl.loop(0, columns // tile)
        def _(n):
            to = pl.ds(pl.multiple_of(n * tile, tile), tile)
            panel = weight[:, pl.ds(pl.multiple_of(side * columns + n * tile, tile), tile)]
            total = jnp.dot(high[...], panel, preferred_element_type=jnp.float32)
            total += jnp.dot(low[...], panel, preferred_element_type=jnp.float32)
            out[side, :, :, to] = total.reshape(layers, width, tile)


def fold_chunk(pieces, weight, sides, layers, width):
    depth, columns = weight.shape
    group = max(1, min(layers, 512 // width))
    return pl.pallas_call(
        fold_kernel,
        out_shape=jax.ShapeDtypeStruct((sides, layers, width, columns // sides), jnp.float32),
        grid=(layers // group,),
        in_specs=[pl.BlockSpec((group * width, pieces[0].shape[1]), lambda step: (step, 0))] * len(pieces)
        + [pl.BlockSpec((depth, columns), lambda step: (0, 0))],
        out_specs=pl.BlockSpec((sides, group, width, columns // sides), lambda step: (0, step, 0, 0)),
        scratch_shapes=[pltpu.VMEM((group * width, depth), jnp.bfloat16)] * 2,
        compiler_params=pltpu.CompilerParams(vmem_limit_bytes=60 * 1024 * 1024),
        cost_estimate=pl.CostEstimate(
            flops=4 * layers * width * depth * columns,
            bytes_accessed=4 * layers * width * (depth + columns) + 2 * depth * columns,
            transcendentals=0,
        ),
    )(*pieces, weight)


def shards(rows_n, ta_n, rotation, query_weight, key_weight, value_weight, head_rotation):
    r, t = lax.axis_index("row"), lax.axis_index("ta")
    low_n = ta_n // 2
    y, x = r % 2, t // low_n
    layers = rows_n // 2
    out_rows = rotation.shape[1] // rows_n
    half = out_rows // 2
    chunks = min(CHUNKS, half // LANES)
    width = half // chunks
    depth = rotation.shape[0]
    everyone = [(a, b) for a in range(rows_n) for b in range(ta_n)]

    def swap(value, row_bit, ta_bit):
        pairs = [(a * ta_n + b, (a ^ row_bit) * ta_n + (b ^ ta_bit)) for a, b in everyone]
        return lax.ppermute(value, ("row", "ta"), pairs)

    weights = (query_weight, key_weight, value_weight)
    shares = [weight.shape[1] // ta_n for weight in weights]
    columns = []
    for low in range(low_n):
        for high in range(2):
            for weight, share in zip(weights, shares):
                owner = high * low_n + low
                columns.append(lax.slice_in_dim(weight, owner * share, (owner + 1) * share, axis=1))
    mine = jnp.concatenate(columns, axis=1)
    weight = jnp.concatenate([mine if o == (0, 0) else swap(mine, o[0], o[1] * low_n) for o in OFFSETS], axis=0)

    place = jnp.stack([y, x]).astype(jnp.int32)
    ta_bits = [1 << b for b in range(low_n.bit_length() - 1)]
    row_bits = [1 << b for b in range(1, rows_n.bit_length() - 1)]
    share_all = sum(shares)
    plain = shares[0] + shares[1]

    def finish(chunk):
        pieces = split_chunk(rotation, place, layers, width, chunk, chunks)
        arrived = [p if o == (0, 0) else swap(p, o[0], o[1] * low_n) for p, o in zip(pieces, OFFSETS)]
        part = fold_chunk(arrived, weight, low_n, layers, width)
        for bits, index, axis in ((ta_bits, t, "ta"), (row_bits, r, "row")):
            for bit in bits:
                part = part.reshape((part.shape[0] // 2, 2) + part.shape[1:])
                own = (index // bit) % 2
                kept = lax.dynamic_index_in_dim(part, own, 1, keepdims=False)
                sent = lax.dynamic_index_in_dim(part, 1 - own, 1, keepdims=False)
                got = swap(sent, bit if axis == "row" else 0, bit if axis == "ta" else 0)
                part = kept + got
            part = part.reshape(part.shape[1:])
        kept = lax.dynamic_slice_in_dim(part, x * share_all, share_all, 1)
        sent = lax.dynamic_slice_in_dim(part, (1 - x) * share_all, share_all, 1)
        return (
            (kept[:, :plain].astype(jnp.bfloat16), kept[:, plain:]),
            (swap(sent[:, :plain].astype(jnp.bfloat16), 0, low_n), swap(sent[:, plain:], 0, low_n)),
        )

    done = [finish(chunk) for chunk in range(chunks)]
    rows = []
    for kind in range(2):
        own = [d[0][kind] for d in done]
        other = [d[1][kind] for d in done]
        rows.append(
            jnp.where(x == 0, jnp.concatenate(own + other, axis=0), jnp.concatenate(other + own, axis=0))
        )
    query_key, value = rows
    heads = value.reshape(value.shape[0], head_rotation.shape[0], head_rotation.shape[1])
    turned = jnp.einsum("jhd,hde->jhe", heads, head_rotation, precision=lax.Precision.HIGHEST)
    value_rotated = turned.reshape(value.shape).astype(jnp.bfloat16)
    return query_key[:, : shares[0]], query_key[:, shares[0] :], value_rotated


def solution(mesh):
    return jax.shard_map(
        functools.partial(shards, mesh.shape["row"], mesh.shape["ta"]),
        mesh=mesh,
        in_specs=(
            P(("row", "ta"), None),
            P(("row", "ta"), None),
            P(("row", "ta"), None),
            P(("row", "ta"), None),
            P("ta", None, None),
        ),
        out_specs=(P("row", "ta"), P("row", "ta"), P("row", "ta")),
        check_vma=False,
    )
```

```python
import functools

import jax
import jax.numpy as jnp
from jax import lax
from jax.experimental import pallas as pl
from jax.experimental.pallas import tpu as pltpu
from jax.sharding import PartitionSpec as P

CHUNKS = 8
LANES = 128
OFFSETS = ((0, 0), (0, 1), (1, 0), (1, 1))


def split_kernel(place, *refs):
    count = len(refs) // 2
    for source, out in zip(refs[:count], refs[count:]):
        block = source[...].T
        depth = block.shape[1]
        high = block.astype(jnp.bfloat16)
        out[:, :depth] = high
        out[:, depth:] = (block - high.astype(jnp.float32)).astype(jnp.bfloat16)


def split_chunk(rotation, place, layers, width, chunk, chunks):
    depth = rotation.shape[0]

    def incoming(dy, dx):
        def index(layer, place):
            y = (place[0] + dy) % 2
            x = (place[1] + dx) % 2
            return 0, ((layer * 2 + y) * 2 + x) * chunks + chunk

        return pl.BlockSpec((depth, width), index)

    return pl.pallas_call(
        split_kernel,
        out_shape=[jax.ShapeDtypeStruct((layers * width, 2 * depth), jnp.bfloat16)] * len(OFFSETS),
        grid_spec=pltpu.PrefetchScalarGridSpec(
            num_scalar_prefetch=1,
            grid=(layers,),
            in_specs=[incoming(*offset) for offset in OFFSETS],
            out_specs=[pl.BlockSpec((width, 2 * depth), lambda layer, place: (layer, 0))] * len(OFFSETS),
        ),
        cost_estimate=pl.CostEstimate(
            flops=0, bytes_accessed=8 * len(OFFSETS) * layers * width * depth, transcendentals=0
        ),
    )(place, *([rotation] * len(OFFSETS)))


def fold_kernel(*refs):
    count = len(OFFSETS)
    pieces, weight, out, high, low = refs[:count], refs[count], refs[count + 1], refs[count + 2], refs[count + 3]
    depth = weight.shape[0] // count
    for n, piece in enumerate(pieces):
        high[:, n * depth : (n + 1) * depth] = piece[:, :depth]
        low[:, n * depth : (n + 1) * depth] = piece[:, depth:]
    sides, layers, width, columns = out.shape
    tile = 2 * LANES if columns % (2 * LANES) == 0 else LANES
    for side in range(sides):

        @pl.loop(0, columns // tile)
        def _(n):
            to = pl.ds(pl.multiple_of(n * tile, tile), tile)
            panel = weight[:, pl.ds(pl.multiple_of(side * columns + n * tile, tile), tile)]
            total = jnp.dot(high[...], panel, preferred_element_type=jnp.float32)
            total += jnp.dot(low[...], panel, preferred_element_type=jnp.float32)
            out[side, :, :, to] = total.reshape(layers, width, tile)


def fold_chunk(pieces, weight, sides, layers, width):
    depth, columns = weight.shape
    group = max(1, min(layers, 512 // width))
    return pl.pallas_call(
        fold_kernel,
        out_shape=jax.ShapeDtypeStruct((sides, layers, width, columns // sides), jnp.float32),
        grid=(layers // group,),
        in_specs=[pl.BlockSpec((group * width, pieces[0].shape[1]), lambda step: (step, 0))] * len(pieces)
        + [pl.BlockSpec((depth, columns), lambda step: (0, 0))],
        out_specs=pl.BlockSpec((sides, group, width, columns // sides), lambda step: (0, step, 0, 0)),
        scratch_shapes=[pltpu.VMEM((group * width, depth), jnp.bfloat16)] * 2,
        compiler_params=pltpu.CompilerParams(vmem_limit_bytes=60 * 1024 * 1024),
        cost_estimate=pl.CostEstimate(
            flops=4 * layers * width * depth * columns,
            bytes_accessed=4 * layers * width * (depth + columns) + 2 * depth * columns,
            transcendentals=0,
        ),
    )(*pieces, weight)


def shards(rows_n, ta_n, rotation, query_weight, key_weight, value_weight, head_rotation):
    r, t = lax.axis_index("row"), lax.axis_index("ta")
    low_n = ta_n // 2
    y, x = r % 2, t // low_n
    layers = rows_n // 2
    out_rows = rotation.shape[1] // rows_n
    half = out_rows // 2
    chunks = min(CHUNKS, half // LANES)
    width = half // chunks
    depth = rotation.shape[0]
    everyone = [(a, b) for a in range(rows_n) for b in range(ta_n)]

    def swap(value, row_bit, ta_bit):
        pairs = [(a * ta_n + b, (a ^ row_bit) * ta_n + (b ^ ta_bit)) for a, b in everyone]
        return lax.ppermute(value, ("row", "ta"), pairs)

    weights = (query_weight, key_weight, value_weight)
    shares = [weight.shape[1] // ta_n for weight in weights]
    columns = []
    for low in range(low_n):
        for high in range(2):
            for weight, share in zip(weights, shares):
                owner = high * low_n + low
                columns.append(lax.slice_in_dim(weight, owner * share, (owner + 1) * share, axis=1))
    mine = jnp.concatenate(columns, axis=1)
    weight = jnp.concatenate([mine if o == (0, 0) else swap(mine, o[0], o[1] * low_n) for o in OFFSETS], axis=0)

    place = jnp.stack([y, x]).astype(jnp.int32)
    ta_bits = [1 << b for b in range(low_n.bit_length() - 1)]
    row_bits = [1 << b for b in range(1, rows_n.bit_length() - 1)]
    share_all = sum(shares)
    plain = shares[0] + shares[1]

    log = [[] for _ in range(chunks)]

    def finish(chunk):
        pieces = split_chunk(rotation, place, layers, width, chunk, chunks)
        arrived = [p if o == (0, 0) else swap(p, o[0], o[1] * low_n) for p, o in zip(pieces, OFFSETS)]
        stages = len(ta_bits) + len(row_bits)
        earlier = [log[chunk - n - 1][n] for n in range(stages) if n < chunk]
        *arrived, _ = lax.optimization_barrier((*arrived, earlier))
        part = fold_chunk(arrived, weight, low_n, layers, width)
        for bits, index, axis in ((ta_bits, t, "ta"), (row_bits, r, "row")):
            for bit in bits:
                part = part.reshape((part.shape[0] // 2, 2) + part.shape[1:])
                own = (index // bit) % 2
                kept = lax.dynamic_index_in_dim(part, own, 1, keepdims=False)
                sent = lax.dynamic_index_in_dim(part, 1 - own, 1, keepdims=False)
                got = swap(sent, bit if axis == "row" else 0, bit if axis == "ta" else 0)
                part = kept + got
                log[chunk].append(part)
            part = part.reshape(part.shape[1:])
        kept = lax.dynamic_slice_in_dim(part, x * share_all, share_all, 1)
        sent = lax.dynamic_slice_in_dim(part, (1 - x) * share_all, share_all, 1)
        return (
            (kept[:, :plain].astype(jnp.bfloat16), kept[:, plain:]),
            (swap(sent[:, :plain].astype(jnp.bfloat16), 0, low_n), swap(sent[:, plain:], 0, low_n)),
        )

    done = [finish(chunk) for chunk in range(chunks)]
    rows = []
    for kind in range(2):
        own = [d[0][kind] for d in done]
        other = [d[1][kind] for d in done]
        rows.append(
            jnp.where(x == 0, jnp.concatenate(own + other, axis=0), jnp.concatenate(other + own, axis=0))
        )
    query_key, value = rows
    heads = value.reshape(value.shape[0], head_rotation.shape[0], head_rotation.shape[1])
    turned = jnp.einsum("jhd,hde->jhe", heads, head_rotation, precision=lax.Precision.HIGHEST)
    value_rotated = turned.reshape(value.shape).astype(jnp.bfloat16)
    return query_key[:, : shares[0]], query_key[:, shares[0] :], value_rotated


def solution(mesh):
    return jax.shard_map(
        functools.partial(shards, mesh.shape["row"], mesh.shape["ta"]),
        mesh=mesh,
        in_specs=(
            P(("row", "ta"), None),
            P(("row", "ta"), None),
            P(("row", "ta"), None),
            P(("row", "ta"), None),
            P("ta", None, None),
        ),
        out_specs=(P("row", "ta"), P("row", "ta"), P("row", "ta")),
        check_vma=False,
    )
```
